32 devices in a mesh: arcs: 8 (over y, x, core), tiles: 4 (over z).
Axes of the slice: x: 2, y: 2, z: 4, core: 2. Of those that a mesh axis runs over, the one named last changes fastest.
Arguments:
- design: bfloat16 [12288, 8192], P('arcs', 'tiles'), may hold values from -0.09375 to 0.09375
- observations: float32 [12288], P('arcs'), may hold values from -25 to 25
- solution: float32 [8192], P('tiles'), may hold values from -6 to 6
- arc_ids: int32 [8, 1536], P('arcs'), may hold values from 0 to 3, never falling along the last dimension, each value on 1 to 768 neighbouring positions
- block_live: int32 [8, 12], P('arcs'), may hold values 0 or 1
Outputs:
- normal: float32 [8192, 8192], P('arcs', 'tiles')
- rhs: float32 [8192], P('tiles')
The draws below stay inside these ranges and needn't reach their ends.
Inputs may be any that keep to these rules, and one draw needn't show every extreme that they name: `arc_ids`: the arcs of a group's rows never fall along its rows; an arc holds at most 768 rows and some arc exactly that many.
All inputs are finite; a program needn't handle non-finite values. No bound on the sum of `block_live` on one device may be relied on, other than what follows from the above.
Results may differ from the reference program's by a relative error of at most 0.0018.
Values may be sent and summed in bfloat16 or wider, within the bound.
A program may use at most 192 MiB of HBM per device.

```python
import math
import jax
import jax.numpy as jnp
import numpy as np
from jax import lax

COEF = 8192
ROWS_DEV = 1536
ARCS_DEV = 4
SEG_MOST = 768
BLOCKS = 12
TOTAL_ROWS = 12288
N_ARCS = 8


def draw_observations(key, part):
    first_key, second_key = jax.random.split(jax.random.fold_in(key, 11))
    position = jnp.arange(TOTAL_ROWS, dtype=jnp.int32)
    denominator = max(TOTAL_ROWS // ROWS_DEV - 1, 1)
    device_frac = (position // ROWS_DEV).astype(jnp.float32) / denominator
    group_scale = jnp.exp(jax.random.uniform(second_key, (TOTAL_ROWS // 64,), minval=-0.5, maxval=0.5))
    local_scale = jnp.repeat(group_scale, 64)
    noise = jnp.clip(jax.random.normal(first_key, (TOTAL_ROWS,)), -5.0, 5.0)
    return (noise * (1.0 + 2.0 * device_frac) * local_scale).astype(jnp.float32)


def set_ends(result, stream_key, low, high):
    index_at = [jax.random.randint(jax.random.fold_in(stream_key, axis), (), 0, length) for axis, length in enumerate(result.shape)]
    longest = result.shape.index(max(result.shape))
    neighbour = index_at[:longest] + [(index_at[longest] + 1) % result.shape[longest]] + index_at[longest + 1:]
    return result.at[tuple(index_at)].set(low).at[tuple(neighbour)].set(high)


def raised(drawn, stream_key, source, target, parts, factor):
    owner, partner = [(jnp.arange(drawn.shape[dim]) // (drawn.shape[dim] // parts)).reshape([-1 if axis == dim else 1 for axis in range(drawn.ndim)]) for dim in (source, target)]
    chosen = jax.random.permutation(stream_key, parts)[partner]
    strong = (owner == chosen) | (owner == (partner + parts // 2) % parts)
    return jnp.where(strong, factor * drawn, drawn)


def shard_levels(own_key, dims, cuts, low, largest):
    def one(dim, blocks):
        steps = jax.random.uniform(jax.random.fold_in(jax.random.fold_in(own_key, 6), dim), (blocks,), jnp.float32, low / len(cuts), largest / len(cuts))
        return jnp.repeat(jnp.exp(steps), dims[dim] // blocks).reshape((-1,) + (1,) * (len(dims) - dim - 1))

    level = one(*cuts[0])
    for cut in cuts[1:]:
        level = level * one(*cut)
    return level


def split_up(number_of, total, bound, skew):
    portions = [(1 << 20) // math.isqrt(standing ** skew) + 1 for standing in range(2, number_of + 1)]
    spare, holding = total - bound - (number_of - 1), [1] * (number_of - 1)
    while spare > 0:
        free = [i for i in range(number_of - 1) if holding[i] < bound]
        whole, budget = sum([portions[i] for i in free]), spare
        for i in free:
            more = min(bound - holding[i], max(1, budget * portions[i] // whole), spare)
            holding[i] = holding[i] + more
            spare = spare - more
    return np.array([bound] + holding)


def uneven(own_key, amount, total, most, skew):
    if amount == 2:
        one = jax.random.randint(own_key, (), max(1, total - most), min(most, total - 1) + 1)
        return jnp.stack([one, total - one])
    tallies = jnp.asarray(split_up(amount, total, most, skew), jnp.int32)
    twos = (amount - 1) // 2
    giver, receiver = tallies[1:1 + 2 * twos:2], tallies[2:2 + 2 * twos:2]
    margin = jnp.minimum(giver - 1, most - receiver)
    moved = jax.random.randint(jax.random.fold_in(own_key, 1), (twos,), 0, 1 << 20) % (margin + 1)
    tallies = tallies.at[1:1 + 2 * twos:2].set(giver - moved).at[2:2 + 2 * twos:2].set(receiver + moved)
    return tallies[jax.random.permutation(jax.random.fold_in(own_key, 2), amount)]


def gaussian(rng, shape, width, reach, cuts=(), kind=jnp.bfloat16):
    values = jax.random.normal(rng, shape, jnp.float32) * width
    if len(cuts) > 0:
        values = shard_levels(rng, shape, cuts, -0.22, 0.18) * values
    return jnp.clip(values, min=-reach, max=reach).astype(kind)


def gaussian_with(own_key, shape, width, limit, pieces, heavy, kind=jnp.bfloat16):
    entries = width * jax.random.normal(own_key, shape, jnp.float32)
    if pieces:
        entries = entries * shard_levels(own_key, shape, pieces, -0.22, 0.18)
    return jnp.clip(raised(entries, jax.random.fold_in(own_key, 3), *heavy), -limit, limit).astype(kind)


def setup_inputs(seed: int = 0) -> dict:
    key_of = jax.random.split(jax.random.key(seed), 6)
    design = gaussian_with(key_of[0], (TOTAL_ROWS, COEF), COEF ** -0.5, 0.09375, ((0, 8), (1, 4)), (0, 1, 8, 2.0))
    observations = draw_observations(jax.random.fold_in(key_of[5], 71), 0)
    solution = gaussian(key_of[2], (COEF,), 1.0, 6.0, ((0, 4),), jnp.float32)
    arc_ids = jax.vmap(lambda own: jnp.searchsorted(jnp.cumsum(uneven(own, ARCS_DEV, ROWS_DEV, SEG_MOST, 2)), jnp.arange(ROWS_DEV), side="right"))(jax.random.split(key_of[3], N_ARCS)).reshape((N_ARCS, ROWS_DEV)).astype(jnp.int32)
    block_live = set_ends((jax.random.randint(key_of[4], (N_ARCS, BLOCKS), 0, 4) < 3).astype(jnp.int32), jax.random.fold_in(key_of[4], 1), 0, 1)
    return {"design": design, "observations": observations, "solution": solution, "arc_ids": arc_ids, "block_live": block_live}


prior_rows = 4.0


def reference(design, observations, solution, arc_ids, block_live):
    groups = arc_ids.shape[0]
    per_group = arc_ids.shape[1]
    row_count = groups * per_group
    live_row = jnp.broadcast_to(block_live[:, :, None], (groups, block_live.shape[1], 128)).reshape(row_count).astype(jnp.float32)
    design_wide = design.astype(jnp.float32)
    predicted = jnp.dot(design_wide, solution, precision=lax.Precision.HIGHEST)
    residual = observations - predicted
    squares = (live_row * residual * residual).reshape(groups, per_group)
    live_group = live_row.reshape(groups, per_group)
    arc_match = (arc_ids[:, None, :] == jnp.arange(ARCS_DEV, dtype=jnp.int32)[None, :, None]).astype(jnp.float32)
    arc_squares = jnp.sum(arc_match * squares[:, None, :], axis=2)
    arc_counts = jnp.sum(arc_match * live_group[:, None, :], axis=2)
    variance_all = (jnp.sum(arc_squares) + 1.0) / (jnp.sum(arc_counts) + 1.0)
    arc_weight = variance_all / ((arc_squares + prior_rows * variance_all) / (arc_counts + prior_rows))
    row_weight = live_row * jnp.sum(arc_match * arc_weight[:, :, None], axis=1).reshape(row_count)
    weighted = (row_weight[:, None] * design_wide).astype(jnp.bfloat16)
    normal = jnp.dot(design_wide.T, weighted.astype(jnp.float32), precision=lax.Precision.HIGHEST)
    rhs = jnp.dot(design_wide.T, row_weight * residual, precision=lax.Precision.HIGHEST)
    return normal, rhs
```

```python
import jax
import jax.numpy as jnp
from jax import lax
from jax.sharding import PartitionSpec as P

ARCS_DEV = 4
CHUNKS = 4

prior_rows = 4.0


def contract_rows(left, right):
    return lax.dot_general(
        left, right, (((0,), (0,)), ((), ())), preferred_element_type=jnp.float32
    )


def row_terms(design, observations, solution, arc_ids, block_live):
    row_count = design.shape[0]
    partial_value = jnp.dot(design.astype(jnp.float32), solution, precision=lax.Precision.HIGHEST)
    predicted = lax.psum(partial_value, "tiles")
    residual = observations - predicted
    live_row = (
        jnp.broadcast_to(block_live[0][:, None], (block_live.shape[1], 128))
        .reshape(row_count)
        .astype(jnp.float32)
    )
    arc_match = (arc_ids[0][None, :] == jnp.arange(ARCS_DEV, dtype=jnp.int32)[:, None]).astype(
        jnp.float32
    )
    squares = live_row * residual * residual
    arc_squares = jnp.sum(arc_match * squares[None, :], axis=1)
    arc_counts = jnp.sum(arc_match * live_row[None, :], axis=1)
    totals = lax.psum(jnp.stack([jnp.sum(arc_squares), jnp.sum(arc_counts)]), "arcs")
    variance_all = (totals[0] + 1.0) / (totals[1] + 1.0)
    arc_weight = variance_all / (
        (arc_squares + prior_rows * variance_all) / (arc_counts + prior_rows)
    )
    row_weight = live_row * jnp.sum(arc_match * arc_weight[:, None], axis=0)
    rhs_part = lax.dot_general(
        design.astype(jnp.float32),
        row_weight * residual,
        (((0,), (0,)), ((), ())),
        precision=lax.Precision.HIGHEST,
    )
    return row_weight, lax.psum(rhs_part, "arcs")


def general(design, observations, solution, arc_ids, block_live):
    design_all = lax.all_gather(design, "tiles", axis=1, tiled=True)
    row_weight, rhs = row_terms(design, observations, solution, arc_ids, block_live)
    weighted = (row_weight[:, None] * design).astype(jnp.bfloat16)
    normal = lax.psum_scatter(
        contract_rows(design_all, weighted), "arcs", scatter_dimension=0, tiled=True
    )
    return (normal, rhs)


def paired(n_arcs, design, observations, solution, arc_ids, block_live):
    n_tiles = n_arcs // 2
    me, z = lax.axis_index("arcs"), lax.axis_index("tiles")
    core, chip = lax.rem(me, 2), lax.div(me, 2)

    def swap(value, bit):
        return lax.ppermute(value, "arcs", [(i, i ^ bit) for i in range(n_arcs)])

    def shift(value, step):
        return lax.ppermute(value, "tiles", [(i, (i + step) % n_tiles) for i in range(n_tiles)])

    over_core, over_x, over_y = 1, 2, 4
    both = jnp.concatenate([design, swap(design, over_core)], axis=0)
    rows, columns = both.shape
    half = columns // 2
    left = lax.dynamic_slice_in_dim(both, core * half, half, 1)
    width = half // CHUNKS

    design, first = lax.optimization_barrier((design, left[:, :width]))
    row_weight, rhs = row_terms(design, observations, solution, arc_ids, block_live)
    row_weight_both = jnp.concatenate([row_weight, swap(row_weight, over_core)])
    weighted = (row_weight_both[:, None] * both).astype(jnp.bfloat16)
    right = (weighted[:, :half], weighted[:, half:])

    pieces = []
    below = above = first
    for h in range(CHUNKS):
        own = first if h == 0 else left[:, h * width : (h + 1) * width]
        if h > 0:
            own, below, above = lax.optimization_barrier((own, below, above))
        below = shift(own, 1)
        above = shift(own, -1)
        far_top = shift(below[: rows // 2], 1)
        far_bottom = shift(above[rows // 2 :], -1)
        gathered = jnp.concatenate([own, above, far_top, far_bottom, below], axis=0).reshape(
            n_tiles, rows, width
        )

        def product(bits, side):
            place = lax.rem((chip ^ bits) - z + n_tiles, n_tiles)
            block = lax.dynamic_index_in_dim(gathered, place, 0, keepdims=False)
            return contract_rows(block, right[side])

        def send(value, bit):
            return swap(value.astype(jnp.bfloat16), bit)

        x_bit, y_bit = over_x // 2, over_y // 2
        a_far = send(product(x_bit | y_bit, 0), over_x)
        b_far = send(product(x_bit | y_bit, 1), over_y)
        a_near = send(product(x_bit, 0), over_x)
        b_near = send(product(y_bit, 1), over_y)
        a_last = send(product(y_bit, 0) + a_far.astype(jnp.float32), over_y)
        b_last = send(product(x_bit, 1) + b_far.astype(jnp.float32), over_x)
        a = product(0, 0) + a_near.astype(jnp.float32) + a_last.astype(jnp.float32)
        b = product(0, 1) + b_near.astype(jnp.float32) + b_last.astype(jnp.float32)
        pieces.append(jnp.concatenate([a, b], axis=1))
    return (jnp.concatenate(pieces, axis=0), rhs)


def solution(mesh):
    n_arcs, n_tiles = mesh.shape["arcs"], mesh.shape["tiles"]

    def local(*args):
        if n_arcs == 2 * n_tiles and n_tiles == 4:
            return paired(n_arcs, *args)
        return general(*args)

    return jax.shard_map(
        local,
        mesh=mesh,
        in_specs=(P("arcs", "tiles"), P("arcs"), P("tiles"), P("arcs", None), P("arcs", None)),
        out_specs=(P("arcs", "tiles"), P("tiles")),
        check_vma=False,
    )
```
